32 devices in a mesh: occ: 4 (over y, x), vir: 8 (over z, core).
Axes of the slice: x: 2, y: 2, z: 4, core: 2. Of those that a mesh axis runs over, the one named last changes fastest.
Arguments:
- b_factors: float32 [32, 256, 4096], P('occ', 'vir'), may hold values from -0.6 to 0.6
- occ_energy: float32 [32], replicated, may hold values from -2 to -0.3
- vir_energy: float32 [256], replicated, may hold values from 0.2 to 3
Outputs:
- gamma: float32 [32, 256, 4096], P('occ', 'vir')
The draws below stay inside these ranges and needn't reach their ends.
All inputs are finite; a program needn't handle non-finite values.
Results may differ from the reference program's by a relative error of at most 0.0003.
Values sent between devices are 32-bit elements; how exact they have to be, the bound alone decides.
A program may use at most 128 MiB of HBM per device.

```python
import jax
import jax.numpy as jnp
from jax import lax

P_SIZE = 4096
OCC_DEV = 8
VIR_DEV = 32
O = 32
V = 256
N_OCC = 4
N_VIR = 8


def steps_of(own_key, extent, pieces, smallest, top_value):
    loudness, own = 1.0, jax.random.fold_in(own_key, 6)
    for axis_at, blocks in pieces:
        steps = jnp.exp(jax.random.uniform(jax.random.fold_in(own, axis_at), (blocks,), jnp.float32, smallest / len(pieces), top_value / len(pieces)))
        loudness = loudness * jnp.repeat(steps, extent[axis_at] // blocks).reshape([-1 if axis == axis_at else 1 for axis in range(len(extent))])
    return loudness


def bell_draw(stream_key, dims, spread, bound, pieces=(), kind=jnp.bfloat16):
    values = spread * jax.random.normal(stream_key, dims, jnp.float32)
    if pieces:
        values = values * steps_of(stream_key, dims, pieces, -0.22, 0.18)
    return jnp.clip(values, -bound, bound).astype(kind)


def setup_inputs(seed: int = 0) -> dict:
    key_list = jax.random.split(jax.random.key(seed), 4)
    b_factors = bell_draw(key_list[0], (O, V, P_SIZE), 0.1, 0.6, ((0, 4), (1, 8)), jnp.float32)
    occ_energy = jnp.clip(jax.random.uniform(key_list[1], (O,), jnp.float32, -2.0, -0.3), -2.0, -0.3)
    vir_energy = jnp.clip(jax.random.uniform(key_list[2], (V,), jnp.float32, 0.2, 3.0), 0.2, 3.0)
    return {"b_factors": b_factors, "occ_energy": occ_energy, "vir_energy": vir_energy}


def reference(b_factors, occ_energy, vir_energy):
    rows = OCC_DEV * VIR_DEV
    width = b_factors.shape[2]
    blocks = b_factors.reshape(N_OCC, OCC_DEV, N_VIR, VIR_DEV, width).transpose(0, 2, 1, 3, 4).reshape(N_OCC, N_VIR, rows, width)
    gaps = (occ_energy[:, None] - vir_energy[None, :]).reshape(N_OCC, OCC_DEV, N_VIR, VIR_DEV).transpose(0, 2, 1, 3).reshape(N_OCC, N_VIR, rows)
    offsets = [(0, 0), (1, 0), (-1, 0), (0, 1), (0, -1)]
    high = lax.Precision.HIGHEST

    def one_block_row(index):
        mine = blocks[index]
        mine_gap = gaps[index]
        total = jnp.zeros_like(mine)
        for shift_occ, shift_vir in offsets:
            other_index = (index + shift_occ) % N_OCC
            other = jnp.roll(blocks[other_index], -shift_vir, axis=0)
            other_gap = jnp.roll(gaps[other_index], -shift_vir, axis=0)
            integral = jnp.einsum("vrp,vsp->vrs", mine, other, precision=high)
            amplitude = integral / (mine_gap[:, :, None] + other_gap[:, None, :])
            total = total + jnp.einsum("vrs,vsp->vrp", amplitude, other, precision=high)
        return total

    result = lax.map(one_block_row, jnp.arange(N_OCC, dtype=jnp.int32))
    return result.reshape(N_OCC, N_VIR, OCC_DEV, VIR_DEV, width).transpose(0, 2, 1, 3, 4).reshape(N_OCC * OCC_DEV, N_VIR * VIR_DEV, width)
```

```python
import functools

import jax
import jax.numpy as jnp
from jax import lax
from jax.experimental import pallas as pl
from jax.experimental.pallas import tpu as pltpu
from jax.sharding import PartitionSpec as P

MESH = pl.DeviceIdType.MESH
CHUNK = 512
STREAMS = 4
SHARES = (4, 4, 4, 8, 16, 16)
LAGS = (2, 2, 2, 3, 6, 6)
RELAY_ROWS = 32
WIDE = 2
DEPTH = 256
STACK = 4


def phases(rows):
    out, base = [], 0
    for share in SHARES:
        count = rows // share
        lanes = STREAMS * count
        out.append((base, count, STACK if STACK * lanes <= DEPTH else 1))
        base += count
    assert base == rows
    return out


def split(value):
    high = value.astype(jnp.bfloat16)
    low = (value - high.astype(jnp.float32)).astype(jnp.bfloat16)
    return high, low


def dot(a, b, contract):
    dims = ((contract[:1], contract[1:]), ((), ()))
    return lax.dot_general(a, b, dimension_numbers=dims, preferred_element_type=jnp.float32)


def product(a, b, contract):
    (a_high, a_low), (b_high, b_low) = a, b
    return dot(a_high, b_high, contract) + (dot(a_high, b_low, contract) + dot(a_low, b_high, contract))


def stacked(amp, block):
    high, low = split(block)
    return dot(amp, jnp.concatenate([high, low] * (STACK // 2), axis=0), (1, 0))


def cols(k, wide=1):
    size = wide * CHUNK
    return pl.ds(pl.multiple_of(k * size, size), size)


def every(count, body, first=0):
    def run(k, carry):
        body(k)
        return carry
    lax.fori_loop(first, count, run, 0)


def kernel(
    occ_count, vir_count, occ_block, vir_block,
    occ_ref, vir_ref, b_ref, total, land, amp_high,
    amp_low, own, own_high, own_low, sums, mine_gap, gaps,
    own_sem, near_send, far_send, inner_send, outer_send, near_recv, far_recv, inner_recv, outer_recv,
):
    rows, width = b_ref.shape
    plan = phases(rows)
    chunks = width // CHUNK
    o = lax.axis_index("occ")
    v = lax.axis_index("vir")
    step = 1 - 2 * lax.rem(o, 2)
    partner = o + step
    relay_to = lax.rem(o + 2 * step + occ_count, occ_count)
    relay_from = lax.rem(o - 2 * step + occ_count, occ_count)
    across = lax.rem(o - step + occ_count, occ_count)
    turn = 1 - 2 * lax.rem(v, 2)
    v_inner = v + turn
    v_outer = lax.rem(v - turn + vir_count, vir_count)
    sources = ((partner, v), (o, v_inner), (o, v_outer), (across, v))
    pieces = [max(1, count // RELAY_ROWS) for _, count, _ in plan]
    near_first = [sum(pieces[:p]) * chunks for p in range(len(plan))]

    def mine(p, i, count, where):
        return b_ref.at[pl.ds(plan[p][0] + i * count, count), where]

    def landed(p, stream, i, count, where):
        return land.at[pl.ds(STREAMS * plan[p][0] + stream * plan[p][1] + i * count, count), where]

    def remote(source, target, send_sem, recv_sem, device):
        return pltpu.make_async_remote_copy(
            source, target, send_sem, recv_sem, device_id=device, device_id_type=MESH)

    def near_copy(p, k, i):
        count = plan[p][1] // pieces[p]
        return remote(
            mine(p, i, count, cols(k)), landed(p, 0, i, count, cols(k)),
            near_send, near_recv.at[near_first[p] + k * pieces[p] + i], (partner, v))

    def far_copy(p, k, i, count):
        return remote(
            landed(p, 0, i, count, cols(k)), landed(p, 3, i, count, cols(k)),
            far_send, far_recv.at[p * chunks + k], (relay_to, v))

    def inner_copy(p):
        count = plan[p][1]
        return remote(
            mine(p, 0, count, slice(None)), landed(p, 1, 0, count, slice(None)),
            inner_send, inner_recv.at[p], (o, v_inner))

    def outer_copy(p, c):
        count = plan[p][1]
        return remote(
            mine(p, 0, count, cols(c, WIDE)), landed(p, 2, 0, count, cols(c, WIDE)),
            outer_send, outer_recv.at[p * (chunks // WIDE) + c], (o, v_outer))

    def load(k):
        return pltpu.make_async_copy(b_ref.at[:, cols(k)], own.at[:, cols(k)], own_sem.at[k])

    def send(p):
        def body(c):
            for k in range(WIDE):
                for i in range(pieces[p]):
                    near_copy(p, WIDE * c + k, i).start()
            outer_copy(p, c).start()
        every(chunks // WIDE, body)
        inner_copy(p).start()

    barrier = pltpu.get_barrier_semaphore()
    for device in ((partner, v), (relay_to, v), (relay_from, v), (o, v_inner), (o, v_outer)):
        pl.semaphore_signal(barrier, inc=1, device_id=device, device_id_type=MESH)
    pl.semaphore_wait(barrier, 5)
    send(0)
    every(chunks, lambda k: load(k).start())
    for p in range(1, len(plan)):
        send(p)

    lane = lax.broadcasted_iota(jnp.int32, (8, rows), 1)

    def gap_row(base, count, blocks):
        part = min(count, vir_block)
        within = lax.rem(lane, part)
        virs = jnp.zeros((8, rows), jnp.float32)
        occs = virs
        for stream, (occ, vir) in enumerate(blocks):
            row = virs
            for a in range(part):
                row = jnp.where(within == a, vir_ref[vir * vir_block + base % vir_block + a], row)
            virs = jnp.where(lane >= stream * count, row, virs)
            for i in range(count // part):
                occs = jnp.where(
                    lane >= stream * count + i * part, occ_ref[occ * occ_block + base // vir_block + i], occs)
        return occs - virs

    def whole(row):
        return jnp.broadcast_to(row[:1], (rows, rows))

    own_row = gap_row(0, rows, [(o, v)])
    mine_gap[...] = whole(own_row).T

    def gather(block, k, copies=1):
        lanes = copies * block.shape[0]
        a = (own_high[:, cols(k)], own_low[:, cols(k)])
        b = [jnp.concatenate([part] * copies, axis=0) if copies > 1 else part for part in split(block)]
        sums[:, :lanes] += product(a, b, (1, 1))

    def amplitude(row, lanes, copies=1):
        value = sums[:, :lanes] / (mine_gap[:, :lanes] + whole(row)[:, :lanes])
        high, low = split(value)
        if copies > 1:
            place = lax.rem(lax.broadcasted_iota(jnp.int32, (rows, lanes), 1), lanes)
            wide = high.astype(jnp.float32)
            amp_high[:, :lanes] = jnp.where(place < lanes // 2, wide, value - wide).astype(jnp.bfloat16)
        else:
            amp_high[:, :lanes] = high
            amp_low[:, :lanes] = low
        sums[...] = jnp.zeros_like(sums)

    def spread(block, copies=1):
        lanes = copies * block.shape[0]
        if copies > 1:
            return stacked(amp_high[:, :lanes], block)
        return product((amp_high[:, :lanes], amp_low[:, :lanes]), split(block), (1, 0))

    sums[...] = jnp.zeros_like(sums)

    def own_chunk(k):
        load(k).wait()
        high, low = split(own[:, cols(k)])
        own_high[:, cols(k)] = high
        own_low[:, cols(k)] = low
        gather(own[:, cols(k)], k)

    def block(p, k):
        return land[pl.ds(STREAMS * plan[p][0], STREAMS * plan[p][1]), cols(k)]

    def read_first(p, k):
        if p == 0:
            total[:, cols(k)] = spread(own[:, cols(k)])
        else:
            total[:, cols(k)] += spread(block(p - 1, k), plan[p - 1][2])

    def read_second(p, k):
        far_copy(p, k, 0, plan[p][1]).wait_recv()

        @pl.when(lax.rem(k, WIDE) == 0)
        def _():
            outer_copy(p, k // WIDE).wait_recv()
        gather(block(p, k), k, plan[p][2])

    def finished(p):
        _, count, copies = plan[p]
        amplitude(gaps[p], copies * STREAMS * count, copies)

    def relay(p, k, i):
        near_copy(p, k, i).wait_recv()
        far_copy(p, k, i, plan[p][1] // pieces[p]).start()

    def arrive(p, k, first=None, second=None):
        for i in range(pieces[p]):
            relay(p, k, i)
            if i == 0 and first is not None:
                first()
        if second is not None:
            second()

    half = chunks // 2
    every(half, own_chunk)
    quarter = half + chunks // 4
    arrive(0, 0, lambda: every(quarter, own_chunk, half), lambda: every(chunks, own_chunk, quarter))
    amplitude(own_row, rows)
    for p, (base, count, copies) in enumerate(plan):
        gaps[p] = gap_row(base, count, list(sources) * copies)

    done, runs = 0, []
    for p in range(len(plan)):
        for k in range(1 if p == 0 else 0, chunks):
            due = p * chunks + k - LAGS[p]
            task = None
            if due >= done:
                task = done // chunks, done % chunks - k
                done += 1
            if runs and runs[-1][0] == p and runs[-1][3] == task:
                runs[-1][2] = k + 1
            else:
                runs.append([p, k, k + 1, task])

    for p, first, end, task in runs:
        if task is None:
            every(end, lambda k, p=p: arrive(p, k), first)
            continue
        q, shift = task
        if first + shift == 0:
            inner_copy(q).wait_recv()
        every(end, lambda k, p=p, q=q, shift=shift: arrive(
            p, k, lambda: read_first(q, k + shift), lambda: read_second(q, k + shift)), first)
        if end + shift == chunks:
            finished(q)

    while done < len(plan) * chunks:
        q, first = done // chunks, done % chunks
        if first == 0:
            inner_copy(q).wait_recv()

        def rest(k, q=q):
            read_first(q, k)
            read_second(q, k)
        every(chunks, rest, first)
        finished(q)
        done = (q + 1) * chunks

    sent = land.at[pl.ds(0, rows), :]
    remote(b_ref, sent, near_send, near_recv.at[0], (partner, v)).wait_send()
    remote(b_ref, sent, inner_send, inner_recv.at[0], (o, v_inner)).wait_send()
    remote(b_ref, sent, outer_send, outer_recv.at[0], (o, v_outer)).wait_send()
    remote(sent, sent, far_send, far_recv.at[0], (relay_to, v)).wait_send()


def finish(total, land, amp, out_ref, done, out_sem):
    rows, width = total.shape
    base, count, copies = phases(rows)[-1]
    chunks = width // CHUNK
    lanes = copies * STREAMS * count

    def store(k):
        return pltpu.make_async_copy(done.at[:, cols(k)], out_ref.at[:, cols(k)], out_sem.at[k])

    def tile(k):
        block = land[pl.ds(STREAMS * base, STREAMS * count), cols(k)]
        done[:, cols(k)] = total[:, cols(k)] + stacked(amp[:, :lanes], block)
        store(k).start()

    every(chunks, tile)
    every(chunks, lambda k: store(k).wait())


def local(b_factors, occ_energy, vir_energy):
    occ_block, vir_block, width = b_factors.shape
    occ_count = lax.axis_size("occ")
    vir_count = lax.axis_size("vir")
    rows = occ_block * vir_block
    plan = phases(rows)
    chunks = width // CHUNK
    near = sum(max(1, count // RELAY_ROWS) for _, count, _ in plan) * chunks
    block = pltpu.VMEM((rows, width), jnp.float32)
    half = pltpu.VMEM((rows, width), jnp.bfloat16)
    square = pltpu.VMEM((rows, rows), jnp.float32)
    amp = pltpu.VMEM((rows, rows), jnp.bfloat16)
    vmem = pl.BlockSpec(memory_space=pltpu.VMEM)
    smem = pl.BlockSpec(memory_space=pltpu.SMEM)
    hbm = pl.BlockSpec(memory_space=pl.ANY)
    sems = [pltpu.SemaphoreType.DMA((chunks,))] + [pltpu.SemaphoreType.DMA] * 4 + [
        pltpu.SemaphoreType.DMA((count,))
        for count in (near, len(plan) * chunks, len(plan), len(plan) * chunks // WIDE)]
    parts = pl.pallas_call(
        functools.partial(kernel, occ_count, vir_count, occ_block, vir_block),
        out_shape=[block, pltpu.VMEM((STREAMS * rows, width), jnp.float32), amp],
        in_specs=[smem, smem, hbm],
        out_specs=[vmem] * 3,
        scratch_shapes=[
            amp, block, half, half, square, square, pltpu.VMEM((len(plan), 8, rows), jnp.float32)] + sems,
        compiler_params=pltpu.CompilerParams(
            collective_id=0, has_side_effects=True, vmem_limit_bytes=42 * 2**20),
    )(occ_energy, vir_energy, b_factors.reshape(rows, width))
    out = pl.pallas_call(
        finish,
        out_shape=jax.ShapeDtypeStruct((rows, width), jnp.float32),
        in_specs=[vmem] * 3,
        out_specs=hbm,
        scratch_shapes=[block, pltpu.SemaphoreType.DMA((chunks,))],
        compiler_params=pltpu.CompilerParams(vmem_limit_bytes=10 * 2**20),
    )(*parts)
    return out.reshape(occ_block, vir_block, width)


def solution(mesh):
    in_specs = (P("occ", "vir", None), P(), P())
    out_specs = P("occ", "vir", None)
    return jax.shard_map(local, mesh=mesh, in_specs=in_specs, out_specs=out_specs, check_vma=False)
```

```python
import functools

import jax
import jax.numpy as jnp
from jax import lax
from jax.experimental import pallas as pl
from jax.experimental.pallas import tpu as pltpu
from jax.sharding import PartitionSpec as P

MESH = pl.DeviceIdType.MESH
CHUNK = 512
STREAMS = 4
SHARES = (4, 4, 4, 8, 8)
LAG = 3
RELAY_ROWS = 16
AHEAD = 8
WIDE = 2
DEPTH = 256


def phases(rows):
    out, base = [], 0
    for share in SHARES:
        out.append((base, rows // share))
        base += rows // share
    assert base == rows
    return out


def split(value):
    high = value.astype(jnp.bfloat16)
    low = (value - high.astype(jnp.float32)).astype(jnp.bfloat16)
    return high, low


def dot(a, b, contract):
    dims = ((contract[:1], contract[1:]), ((), ()))
    return lax.dot_general(a, b, dimension_numbers=dims, preferred_element_type=jnp.float32)


def product(a, b, contract):
    (a_high, a_low), (b_high, b_low) = a, b
    return dot(a_high, b_high, contract) + (dot(a_high, b_low, contract) + dot(a_low, b_high, contract))


def spread(amp_high, amp_low, block):
    count = block.shape[0]
    high, low = split(block)
    if 2 * count <= DEPTH:
        return dot(amp_high[:, :2 * count], jnp.concatenate([high, high], axis=0), (1, 0)) + dot(
            amp_high[:, :count], low, (1, 0))
    return product((amp_high[:, :count], amp_low[:, :count]), (high, low), (1, 0))


def cols(k, wide=1):
    size = wide * CHUNK
    return pl.ds(pl.multiple_of(k * size, size), size)


def every(count, body, first=0):
    def run(k, carry):
        body(k)
        return carry
    lax.fori_loop(first, count, run, 0)


def kernel(
    occ_count, vir_count, occ_block, vir_block,
    occ_ref, vir_ref, b_ref, total, land, amp_high, amp_low,
    own, own_high, own_low, sums, mine_gap, gaps,
    own_sem, near_send, far_send, inner_send, outer_send, near_recv, far_recv, inner_recv, outer_recv,
):
    rows, width = b_ref.shape
    plan = phases(rows)
    chunks = width // CHUNK
    o = lax.axis_index("occ")
    v = lax.axis_index("vir")
    step = 1 - 2 * lax.rem(o, 2)
    partner = o + step
    relay_to = lax.rem(o + 2 * step + occ_count, occ_count)
    relay_from = lax.rem(o - 2 * step + occ_count, occ_count)
    across = lax.rem(o - step + occ_count, occ_count)
    turn = 1 - 2 * lax.rem(v, 2)
    v_inner = v + turn
    v_outer = lax.rem(v - turn + vir_count, vir_count)
    sources = ((partner, v), (o, v_inner), (o, v_outer), (across, v))
    pieces = [count // RELAY_ROWS for _, count in plan]
    pairs = [WIDE if count > min(c for _, c in plan) else 1 for _, count in plan]
    far_first = [sum(chunks // pair for pair in pairs[:p]) for p in range(len(plan))]

    def mine(p, i, count, where):
        return b_ref.at[pl.ds(plan[p][0] + i * count, count), where]

    def landed(p, stream, i, count, where):
        return land.at[pl.ds(STREAMS * plan[p][0] + stream * plan[p][1] + i * count, count), where]

    def remote(source, target, send_sem, recv_sem, device):
        return pltpu.make_async_remote_copy(
            source, target, send_sem, recv_sem, device_id=device, device_id_type=MESH)

    def near_copy(p, k, i):
        return remote(
            mine(p, i, RELAY_ROWS, cols(k)), landed(p, 0, i, RELAY_ROWS, cols(k)),
            near_send, near_recv.at[lax.rem(k * pieces[p] + i, 2 * AHEAD)], (partner, v))

    def far_copy(p, k, i):
        return remote(
            landed(p, 0, i, RELAY_ROWS, cols(k)), landed(p, 3, i, RELAY_ROWS, cols(k)),
            far_send, far_recv.at[far_first[p] + k // pairs[p]], (relay_to, v))

    def far_here(p, c):
        where = cols(c, pairs[p])
        return remote(
            landed(p, 0, 0, plan[p][1], where), landed(p, 3, 0, plan[p][1], where),
            far_send, far_recv.at[far_first[p] + c], (relay_to, v))

    def inner_copy(p):
        count = plan[p][1]
        return remote(
            mine(p, 0, count, slice(None)), landed(p, 1, 0, count, slice(None)),
            inner_send, inner_recv.at[p], (o, v_inner))

    def outer_copy(p, c):
        count = plan[p][1]
        return remote(
            mine(p, 0, count, cols(c, WIDE)), landed(p, 2, 0, count, cols(c, WIDE)),
            outer_send, outer_recv.at[p * (chunks // WIDE) + c], (o, v_outer))

    def load(k):
        return pltpu.make_async_copy(b_ref.at[:, cols(k, WIDE)], own.at[:, cols(k, WIDE)], own_sem.at[k])

    barrier = pltpu.get_barrier_semaphore()
    for device in ((partner, v), (relay_to, v), (relay_from, v), (o, v_inner), (o, v_outer)):
        pl.semaphore_signal(barrier, inc=1, device_id=device, device_id_type=MESH)
    pl.semaphore_wait(barrier, 5)
    for n in range(AHEAD):
        near_copy(0, n // pieces[0], n % pieces[0]).start()
    for p in range(len(plan)):
        every(chunks // WIDE, lambda c: outer_copy(p, c).start())
        inner_copy(p).start()
        if p == 0:
            every(chunks // WIDE, lambda k: load(k).start())

    lane = lax.broadcasted_iota(jnp.int32, (8, rows), 1)

    def gap_row(base, count, blocks):
        part = min(count, vir_block)
        within = lax.rem(lane, part)
        virs = jnp.zeros((8, rows), jnp.float32)
        occs = virs
        for stream, (occ, vir) in enumerate(blocks):
            row = virs
            for a in range(part):
                row = jnp.where(within == a, vir_ref[vir * vir_block + base % vir_block + a], row)
            virs = jnp.where(lane >= stream * count, row, virs)
            for i in range(count // part):
                occs = jnp.where(
                    lane >= stream * count + i * part, occ_ref[occ * occ_block + base // vir_block + i], occs)
        return occs - virs

    def whole(row):
        return jnp.broadcast_to(row[:1], (rows, rows))

    own_row = gap_row(0, rows, [(o, v)])
    mine_gap[...] = whole(own_row).T

    def gather(block, k):
        count = block.shape[0]
        mine = (own_high[:, cols(k)], own_low[:, cols(k)])
        sums[:, :count] += product(mine, split(block), (1, 1))

    def amplitude(row, count):
        value = sums[:, :count] / (mine_gap[:, :count] + whole(row)[:, :count])
        high, low = split(value)
        amp_high[:, :count] = high
        if 2 * count <= DEPTH:
            amp_high[:, count:2 * count] = low
        else:
            amp_low[:, :count] = low
        sums[...] = jnp.zeros_like(sums)

    sums[...] = jnp.zeros_like(sums)

    def own_chunk(k):
        @pl.when(lax.rem(k, WIDE) == 0)
        def _():
            load(k // WIDE).wait()
        high, low = split(own[:, cols(k)])
        own_high[:, cols(k)] = high
        own_low[:, cols(k)] = low
        gather(own[:, cols(k)], k)

    def block(p, k):
        return land[pl.ds(STREAMS * plan[p][0], STREAMS * plan[p][1]), cols(k)]

    def read_first(p, k):
        if p == 0:
            total[:, cols(k)] = spread(amp_high, amp_low, own[:, cols(k)])
        else:
            total[:, cols(k)] += spread(amp_high, amp_low, block(p - 1, k))

    def read_second(p, k):
        if pairs[p] == 1:
            far_here(p, k).wait_recv()

        @pl.when(lax.rem(k, WIDE) == 0)
        def _():
            if pairs[p] == WIDE:
                far_here(p, k // WIDE).wait_recv()
            outer_copy(p, k // WIDE).wait_recv()
        gather(block(p, k), k)

    def finished(p):
        amplitude(gaps[p], STREAMS * plan[p][1])

    def relay(p, k, i):
        near_copy(p, k, i).wait_recv()
        far_copy(p, k, i).start()
        later = chunks - AHEAD // pieces[p]

        @pl.when(k < later)
        def _():
            near_copy(p, k + AHEAD // pieces[p], i).start()

        if p + 1 < len(plan):
            ratio = pieces[p] // pieces[p + 1]

            @pl.when(k >= later)
            def _():
                near_copy(p + 1, (k - later) * ratio + i // pieces[p + 1], i % pieces[p + 1]).start()

    def arrive(p, k, work):
        for i in range(pieces[p]):
            relay(p, k, i)
            if i < len(work):
                work[i]()

    def fill(p):
        gaps[p] = gap_row(plan[p][0], plan[p][1], sources)

    assert pieces[0] == 4 and len(plan) == 5
    half = chunks // 2
    every(half, own_chunk)
    arrive(0, 0, [functools.partial(every, half + n + 1, own_chunk, half + n) for n in range(half)])
    arrive(0, 1, [lambda: amplitude(own_row, rows), lambda: fill(0), lambda: fill(1)])
    arrive(0, 2, [lambda: fill(2), lambda: fill(3), lambda: fill(4)])

    done, runs = 0, []
    for p in range(len(plan)):
        for k in range(LAG if p == 0 else 0, chunks):
            due = p * chunks + k - LAG
            task = None
            if due >= done:
                task = done // chunks, done % chunks - k
                done += 1
            if runs and runs[-1][0] == p and runs[-1][3] == task:
                runs[-1][2] = k + 1
            else:
                runs.append([p, k, k + 1, task])

    for p, first, end, task in runs:
        if task is None:
            every(end, lambda k, p=p: arrive(p, k, []), first)
            continue
        q, shift = task
        if first + shift == 0:
            inner_copy(q).wait_recv()
        every(end, lambda k, p=p, q=q, shift=shift: arrive(
            p, k, [lambda: read_first(q, k + shift), lambda: read_second(q, k + shift)]), first)
        if end + shift == chunks:
            finished(q)

    while done < len(plan) * chunks:
        q, first = done // chunks, done % chunks
        if first == 0:
            inner_copy(q).wait_recv()

        def rest(k, q=q):
            read_first(q, k)
            read_second(q, k)
        every(chunks, rest, first)
        finished(q)
        done = (q + 1) * chunks

    sent = land.at[pl.ds(0, rows), :]
    remote(b_ref, sent, near_send, near_recv.at[0], (partner, v)).wait_send()
    remote(b_ref, sent, inner_send, inner_recv.at[0], (o, v_inner)).wait_send()
    remote(b_ref, sent, outer_send, outer_recv.at[0], (o, v_outer)).wait_send()
    remote(sent, sent, far_send, far_recv.at[0], (relay_to, v)).wait_send()


def finish(total, land, amp_high, amp_low, out_ref, done, out_sem):
    rows, width = total.shape
    base, count = phases(rows)[-1]
    stores = []
    for k in range(width // CHUNK):
        where = pl.ds(k * CHUNK, CHUNK)
        block = land[pl.ds(STREAMS * base, STREAMS * count), where]
        done[:, where] = total[:, where] + spread(amp_high, amp_low, block)
        stores.append(pltpu.make_async_copy(done.at[:, where], out_ref.at[:, where], out_sem.at[k]))
        stores[-1].start()
    for store in stores:
        store.wait()


def local(b_factors, occ_energy, vir_energy):
    occ_block, vir_block, width = b_factors.shape
    occ_count = lax.axis_size("occ")
    vir_count = lax.axis_size("vir")
    rows = occ_block * vir_block
    plan = phases(rows)
    chunks = width // CHUNK
    short = min(count for _, count in plan)
    far = sum(chunks if count == short else chunks // WIDE for _, count in plan)
    block = pltpu.VMEM((rows, width), jnp.float32)
    half = pltpu.VMEM((rows, width), jnp.bfloat16)
    square = pltpu.VMEM((rows, rows), jnp.float32)
    amp = pltpu.VMEM((rows, rows), jnp.bfloat16)
    vmem = pl.BlockSpec(memory_space=pltpu.VMEM)
    smem = pl.BlockSpec(memory_space=pltpu.SMEM)
    hbm = pl.BlockSpec(memory_space=pl.ANY)
    sems = [pltpu.SemaphoreType.DMA((chunks // WIDE,))] + [pltpu.SemaphoreType.DMA] * 4 + [
        pltpu.SemaphoreType.DMA((count,))
        for count in (2 * AHEAD, far, len(plan), len(plan) * chunks // WIDE)]
    parts = pl.pallas_call(
        functools.partial(kernel, occ_count, vir_count, occ_block, vir_block),
        out_shape=[block, pltpu.VMEM((STREAMS * rows, width), jnp.float32), amp, amp],
        in_specs=[smem, smem, hbm],
        out_specs=[vmem] * 4,
        scratch_shapes=[
            block, half, half, square, square, pltpu.VMEM((len(plan), 8, rows), jnp.float32)] + sems,
        compiler_params=pltpu.CompilerParams(
            collective_id=0, has_side_effects=True, vmem_limit_bytes=42 * 2**20),
    )(occ_energy, vir_energy, b_factors.reshape(rows, width))
    out = pl.pallas_call(
        finish,
        out_shape=jax.ShapeDtypeStruct((rows, width), jnp.float32),
        in_specs=[vmem] * 4,
        out_specs=hbm,
        scratch_shapes=[block, pltpu.SemaphoreType.DMA((chunks,))],
        compiler_params=pltpu.CompilerParams(vmem_limit_bytes=10 * 2**20),
    )(*parts)
    return out.reshape(occ_block, vir_block, width)


def solution(mesh):
    in_specs = (P("occ", "vir", None), P(), P())
    out_specs = P("occ", "vir", None)
    return jax.shard_map(local, mesh=mesh, in_specs=in_specs, out_specs=out_specs, check_vma=False)
```

```python
import functools

import jax
import jax.numpy as jnp
from jax import lax
from jax.experimental import pallas as pl
from jax.experimental.pallas import tpu as pltpu
from jax.sharding import PartitionSpec as P

MESH = pl.DeviceIdType.MESH
CHUNK = 512
STREAMS = 4
SHARES = (4, 4, 4, 8, 8)
LAG = 4
RELAY_ROWS = 16
AHEAD = 8
EARLY = 0
WIDE = 2
DEPTH = 256


def phases(rows):
    out, base = [], 0
    for share in SHARES:
        out.append((base, rows // share))
        base += rows // share
    assert base == rows
    return out


def split(value):
    high = value.astype(jnp.bfloat16)
    low = (value - high.astype(jnp.float32)).astype(jnp.bfloat16)
    return high, low


def dot(a, b, contract):
    dims = ((contract[:1], contract[1:]), ((), ()))
    return lax.dot_general(a, b, dimension_numbers=dims, preferred_element_type=jnp.float32)


def product(a, b, contract):
    (a_high, a_low), (b_high, b_low) = a, b
    return dot(a_high, b_high, contract) + (dot(a_high, b_low, contract) + dot(a_low, b_high, contract))


def spread(amp_high, amp_low, block):
    count = block.shape[0]
    high, low = split(block)
    if 2 * count <= DEPTH:
        return dot(amp_high[:, :2 * count], jnp.concatenate([high, high], axis=0), (1, 0)) + dot(
            amp_high[:, :count], low, (1, 0))
    return product((amp_high[:, :count], amp_low[:, :count]), (high, low), (1, 0))


def cols(k, wide=1):
    size = wide * CHUNK
    return pl.ds(pl.multiple_of(k * size, size), size)


def every(count, body, first=0):
    def run(k, carry):
        body(k)
        return carry
    lax.fori_loop(first, count, run, 0)


def kernel(
    occ_count, vir_count, occ_block, vir_block,
    occ_ref, vir_ref, b_ref, total, land, amp_high, amp_low,
    own, own_high, own_low, sums, mine_gap, gaps,
    own_sem, near_send, far_send, inner_send, outer_send, near_recv, far_recv, inner_recv, outer_recv,
):
    rows, width = b_ref.shape
    plan = phases(rows)
    chunks = width // CHUNK
    o = lax.axis_index("occ")
    v = lax.axis_index("vir")
    step = 1 - 2 * lax.rem(o, 2)
    partner = o + step
    relay_to = lax.rem(o + 2 * step + occ_count, occ_count)
    relay_from = lax.rem(o - 2 * step + occ_count, occ_count)
    across = lax.rem(o - step + occ_count, occ_count)
    turn = 1 - 2 * lax.rem(v, 2)
    v_inner = v + turn
    v_outer = lax.rem(v - turn + vir_count, vir_count)
    sources = ((partner, v), (o, v_inner), (o, v_outer), (across, v))
    pieces = [count // RELAY_ROWS for _, count in plan]
    pairs = [WIDE if count > min(c for _, c in plan) else 1 for _, count in plan]
    far_first = [sum(chunks // pair for pair in pairs[:p]) for p in range(len(plan))]

    def mine(p, i, count, where, ref=b_ref):
        return ref.at[pl.ds(plan[p][0] + i * count, count), where]

    def landed(p, stream, i, count, where):
        return land.at[pl.ds(STREAMS * plan[p][0] + stream * plan[p][1] + i * count, count), where]

    def remote(source, target, send_sem, recv_sem, device):
        return pltpu.make_async_remote_copy(
            source, target, send_sem, recv_sem, device_id=device, device_id_type=MESH)

    def near_copy(p, k, i, ref=b_ref):
        return remote(
            mine(p, i, RELAY_ROWS, cols(k), ref), landed(p, 0, i, RELAY_ROWS, cols(k)),
            near_send, near_recv.at[lax.rem(k * pieces[p] + i, 2 * AHEAD)], (partner, v))

    def far_copy(p, k, i):
        return remote(
            landed(p, 0, i, RELAY_ROWS, cols(k)), landed(p, 3, i, RELAY_ROWS, cols(k)),
            far_send, far_recv.at[far_first[p] + k // pairs[p]], (relay_to, v))

    def far_here(p, c):
        where = cols(c, pairs[p])
        return remote(
            landed(p, 0, 0, plan[p][1], where), landed(p, 3, 0, plan[p][1], where),
            far_send, far_recv.at[far_first[p] + c], (relay_to, v))

    def inner_copy(p):
        count = plan[p][1]
        return remote(
            mine(p, 0, count, slice(None)), landed(p, 1, 0, count, slice(None)),
            inner_send, inner_recv.at[p], (o, v_inner))

    def outer_copy(p, c):
        count = plan[p][1]
        return remote(
            mine(p, 0, count, cols(c, WIDE)), landed(p, 2, 0, count, cols(c, WIDE)),
            outer_send, outer_recv.at[p * (chunks // WIDE) + c], (o, v_outer))

    def load(k):
        return pltpu.make_async_copy(b_ref.at[:, cols(k, WIDE)], own.at[:, cols(k, WIDE)], own_sem.at[k])

    barrier = pltpu.get_barrier_semaphore()
    for device in ((partner, v), (relay_to, v), (relay_from, v), (o, v_inner), (o, v_outer)):
        pl.semaphore_signal(barrier, inc=1, device_id=device, device_id_type=MESH)
    every(chunks // WIDE, lambda k: load(k).start())
    load(0).wait()
    pl.semaphore_wait(barrier, 5)
    for n in range(AHEAD):
        near_copy(0, n // pieces[0], n % pieces[0], own).start()
    for p in range(len(plan)):
        every(chunks // WIDE, lambda c: outer_copy(p, c).start())
        inner_copy(p).start()

    lane = lax.broadcasted_iota(jnp.int32, (8, rows), 1)

    def gap_row(base, count, blocks):
        part = min(count, vir_block)
        within = lax.rem(lane, part)
        virs = jnp.zeros((8, rows), jnp.float32)
        occs = virs
        for stream, (occ, vir) in enumerate(blocks):
            row = virs
            for a in range(part):
                row = jnp.where(within == a, vir_ref[vir * vir_block + base % vir_block + a], row)
            virs = jnp.where(lane >= stream * count, row, virs)
            for i in range(count // part):
                occs = jnp.where(
                    lane >= stream * count + i * part, occ_ref[occ * occ_block + base // vir_block + i], occs)
        return occs - virs

    def whole(row):
        return jnp.broadcast_to(row[:1], (rows, rows))

    own_row = gap_row(0, rows, [(o, v)])
    mine_gap[...] = whole(own_row).T

    def gather(block, k):
        count = block.shape[0]
        mine = (own_high[:, cols(k)], own_low[:, cols(k)])
        sums[:, :count] += product(mine, split(block), (1, 1))

    def amplitude(row, count):
        value = sums[:, :count] / (mine_gap[:, :count] + whole(row)[:, :count])
        high, low = split(value)
        amp_high[:, :count] = high
        if 2 * count <= DEPTH:
            amp_high[:, count:2 * count] = low
        else:
            amp_low[:, :count] = low
        sums[...] = jnp.zeros_like(sums)

    sums[...] = jnp.zeros_like(sums)

    def own_chunk(k):
        high, low = split(own[:, cols(k)])
        own_high[:, cols(k)] = high
        own_low[:, cols(k)] = low
        gather(own[:, cols(k)], k)

    def block(p, k):
        return land[pl.ds(STREAMS * plan[p][0], STREAMS * plan[p][1]), cols(k)]

    def read_first(p, k):
        if p == 0:
            total[:, cols(k)] = spread(amp_high, amp_low, own[:, cols(k)])
        else:
            total[:, cols(k)] += spread(amp_high, amp_low, block(p - 1, k))

    def read_second(p, k):
        if pairs[p] == 1:
            far_here(p, k).wait_recv()

        @pl.when(lax.rem(k, WIDE) == 0)
        def _():
            if pairs[p] == WIDE:
                far_here(p, k // WIDE).wait_recv()
            outer_copy(p, k // WIDE).wait_recv()
        gather(block(p, k), k)

    def finished(p):
        amplitude(gaps[p], STREAMS * plan[p][1])

    def relay(p, k, i):
        near_copy(p, k, i).wait_recv()
        far_copy(p, k, i).start()
        later = chunks - AHEAD // pieces[p]

        @pl.when(k < later)
        def _():
            near_copy(p, k + AHEAD // pieces[p], i, own).start()

        if p + 1 < len(plan):
            ratio = pieces[p] // pieces[p + 1]

            @pl.when(k >= later)
            def _():
                near_copy(p + 1, (k - later) * ratio + i // pieces[p + 1], i % pieces[p + 1], own).start()

    def arrive(p, k, work):
        for i in range(pieces[p]):
            relay(p, k, i)
            if i < len(work):
                work[i]()

    def fill(p):
        gaps[p] = gap_row(plan[p][0], plan[p][1], sources)

    every(chunks // WIDE, lambda k: load(k).wait(), 1)
    every(EARLY, own_chunk)
    slots = [functools.partial(every, k + 1, own_chunk, k) for k in range(EARLY, chunks)]
    slots += [lambda: amplitude(own_row, rows)] + [functools.partial(fill, p) for p in range(len(plan))]
    for k in range(LAG):
        arrive(0, k, slots[k * pieces[0]:(k + 1) * pieces[0]])
    assert len(slots) <= LAG * pieces[0]

    done, runs = 0, []
    for p in range(len(plan)):
        for k in range(LAG if p == 0 else 0, chunks):
            due = p * chunks + k - LAG
            task = None
            if due >= done:
                task = done // chunks, done % chunks - k
                done += 1
            if runs and runs[-1][0] == p and runs[-1][3] == task:
                runs[-1][2] = k + 1
            else:
                runs.append([p, k, k + 1, task])

    for p, first, end, task in runs:
        if task is None:
            every(end, lambda k, p=p: arrive(p, k, []), first)
            continue
        q, shift = task
        if first + shift == 0:
            inner_copy(q).wait_recv()
        every(end, lambda k, p=p, q=q, shift=shift: arrive(
            p, k, [lambda: read_first(q, k + shift), lambda: read_second(q, k + shift)]), first)
        if end + shift == chunks:
            finished(q)

    while done < len(plan) * chunks:
        q, first = done // chunks, done % chunks
        if first == 0:
            inner_copy(q).wait_recv()

        def rest(k, q=q):
            read_first(q, k)
            read_second(q, k)
        every(chunks, rest, first)
        finished(q)
        done = (q + 1) * chunks

    sent = land.at[pl.ds(0, rows), :]
    remote(b_ref, sent, near_send, near_recv.at[0], (partner, v)).wait_send()
    remote(b_ref, sent, inner_send, inner_recv.at[0], (o, v_inner)).wait_send()
    remote(b_ref, sent, outer_send, outer_recv.at[0], (o, v_outer)).wait_send()
    remote(sent, sent, far_send, far_recv.at[0], (relay_to, v)).wait_send()


def finish(total, land, amp_high, amp_low, out_ref, done, out_sem):
    rows, width = total.shape
    base, count = phases(rows)[-1]
    stores = []
    for k in range(width // CHUNK):
        where = pl.ds(k * CHUNK, CHUNK)
        block = land[pl.ds(STREAMS * base, STREAMS * count), where]
        done[:, where] = total[:, where] + spread(amp_high, amp_low, block)
        stores.append(pltpu.make_async_copy(done.at[:, where], out_ref.at[:, where], out_sem.at[k]))
        stores[-1].start()
    for store in stores:
        store.wait()


def local(b_factors, occ_energy, vir_energy):
    occ_block, vir_block, width = b_factors.shape
    occ_count = lax.axis_size("occ")
    vir_count = lax.axis_size("vir")
    rows = occ_block * vir_block
    plan = phases(rows)
    chunks = width // CHUNK
    short = min(count for _, count in plan)
    far = sum(chunks if count == short else chunks // WIDE for _, count in plan)
    block = pltpu.VMEM((rows, width), jnp.float32)
    half = pltpu.VMEM((rows, width), jnp.bfloat16)
    square = pltpu.VMEM((rows, rows), jnp.float32)
    amp = pltpu.VMEM((rows, rows), jnp.bfloat16)
    vmem = pl.BlockSpec(memory_space=pltpu.VMEM)
    smem = pl.BlockSpec(memory_space=pltpu.SMEM)
    hbm = pl.BlockSpec(memory_space=pl.ANY)
    sems = [pltpu.SemaphoreType.DMA((chunks // WIDE,))] + [pltpu.SemaphoreType.DMA] * 4 + [
        pltpu.SemaphoreType.DMA((count,))
        for count in (2 * AHEAD, far, len(plan), len(plan) * chunks // WIDE)]
    parts = pl.pallas_call(
        functools.partial(kernel, occ_count, vir_count, occ_block, vir_block),
        out_shape=[block, pltpu.VMEM((STREAMS * rows, width), jnp.float32), amp, amp],
        in_specs=[smem, smem, hbm],
        out_specs=[vmem] * 4,
        scratch_shapes=[
            block, half, half, square, square, pltpu.VMEM((len(plan), 8, rows), jnp.float32)] + sems,
        compiler_params=pltpu.CompilerParams(
            collective_id=0, has_side_effects=True, vmem_limit_bytes=42 * 2**20),
    )(occ_energy, vir_energy, b_factors.reshape(rows, width))
    out = pl.pallas_call(
        finish,
        out_shape=jax.ShapeDtypeStruct((rows, width), jnp.float32),
        in_specs=[vmem] * 4,
        out_specs=hbm,
        scratch_shapes=[block, pltpu.SemaphoreType.DMA((chunks,))],
        compiler_params=pltpu.CompilerParams(vmem_limit_bytes=10 * 2**20),
    )(*parts)
    return out.reshape(occ_block, vir_block, width)


def solution(mesh):
    in_specs = (P("occ", "vir", None), P(), P())
    out_specs = P("occ", "vir", None)
    return jax.shard_map(local, mesh=mesh, in_specs=in_specs, out_specs=out_specs, check_vma=False)
```

```python
import functools

import jax
import jax.numpy as jnp
from jax import lax
from jax.experimental import pallas as pl
from jax.experimental.pallas import tpu as pltpu
from jax.sharding import PartitionSpec as P

MESH = pl.DeviceIdType.MESH
CHUNK = 512
STREAMS = 4
SHARES = (4, 4, 4, 8, 8)
LAG = 5
RELAY_ROWS = 16
AHEAD = 8
WIDE = 2
DEPTH = 256


def phases(rows):
    out, base = [], 0
    for share in SHARES:
        out.append((base, rows // share))
        base += rows // share
    assert base == rows
    return out


def split(value):
    high = value.astype(jnp.bfloat16)
    low = (value - high.astype(jnp.float32)).astype(jnp.bfloat16)
    return high, low


def dot(a, b, contract):
    dims = ((contract[:1], contract[1:]), ((), ()))
    return lax.dot_general(a, b, dimension_numbers=dims, preferred_element_type=jnp.float32)


def product(a, b, contract):
    (a_high, a_low), (b_high, b_low) = a, b
    return dot(a_high, b_high, contract) + (dot(a_high, b_low, contract) + dot(a_low, b_high, contract))


def spread(amp_high, amp_low, block):
    count = block.shape[0]
    high, low = split(block)
    if 2 * count <= DEPTH:
        return dot(amp_high[:, :2 * count], jnp.concatenate([high, high], axis=0), (1, 0)) + dot(
            amp_high[:, :count], low, (1, 0))
    return product((amp_high[:, :count], amp_low[:, :count]), (high, low), (1, 0))


def cols(k, wide=1):
    size = wide * CHUNK
    return pl.ds(pl.multiple_of(k * size, size), size)


def every(count, body, first=0):
    def run(k, carry):
        body(k)
        return carry
    lax.fori_loop(first, count, run, 0)


def kernel(
    occ_count, vir_count, occ_block, vir_block,
    occ_ref, vir_ref, b_ref, total, land, amp_high, amp_low,
    own, own_high, own_low, sums, mine_gap, gaps,
    far_free, own_sem, near_send, far_send, inner_send, outer_send, near_recv, far_recv, inner_recv, outer_recv,
):
    rows, width = b_ref.shape
    plan = phases(rows)
    chunks = width // CHUNK
    o = lax.axis_index("occ")
    v = lax.axis_index("vir")
    step = 1 - 2 * lax.rem(o, 2)
    partner = o + step
    relay_to = lax.rem(o + 2 * step + occ_count, occ_count)
    relay_from = lax.rem(o - 2 * step + occ_count, occ_count)
    across = lax.rem(o - step + occ_count, occ_count)
    turn = 1 - 2 * lax.rem(v, 2)
    v_inner = v + turn
    v_outer = lax.rem(v - turn + vir_count, vir_count)
    sources = ((partner, v), (o, v_inner), (o, v_outer), (across, v))
    pieces = [count // RELAY_ROWS for _, count in plan]
    pairs = [WIDE if count > min(c for _, c in plan) else 1 for _, count in plan]
    far_first = [sum(chunks // pair for pair in pairs[:p]) for p in range(len(plan) + 1)]
    reused = far_first[-1] - chunks
    assert chunks in far_first and reused in far_first

    def mine(p, i, count, where, ref=b_ref):
        return ref.at[pl.ds(plan[p][0] + i * count, count), where]

    def landed(p, stream, i, count, where):
        return land.at[pl.ds(STREAMS * plan[p][0] + stream * plan[p][1] + i * count, count), where]

    def remote(source, target, send_sem, recv_sem, device):
        return pltpu.make_async_remote_copy(
            source, target, send_sem, recv_sem, device_id=device, device_id_type=MESH)

    def near_copy(p, k, i, ref=b_ref):
        return remote(
            mine(p, i, RELAY_ROWS, cols(k), ref), landed(p, 0, i, RELAY_ROWS, cols(k)),
            near_send, near_recv.at[lax.rem(k * pieces[p] + i, 2 * AHEAD)], (partner, v))

    def far_copy(p, k, i):
        return remote(
            landed(p, 0, i, RELAY_ROWS, cols(k)), landed(p, 3, i, RELAY_ROWS, cols(k)),
            far_send, far_recv.at[lax.rem(far_first[p] + k // pairs[p], chunks)], (relay_to, v))

    def far_here(p, c):
        where = cols(c, pairs[p])
        return remote(
            landed(p, 0, 0, plan[p][1], where), landed(p, 3, 0, plan[p][1], where),
            far_send, far_recv.at[lax.rem(far_first[p] + c, chunks)], (relay_to, v))

    def inner_copy(p):
        count = plan[p][1]
        return remote(
            mine(p, 0, count, slice(None)), landed(p, 1, 0, count, slice(None)),
            inner_send, inner_recv.at[p], (o, v_inner))

    def outer_copy(p, c):
        count = plan[p][1]
        return remote(
            mine(p, 0, count, cols(c, WIDE)), landed(p, 2, 0, count, cols(c, WIDE)),
            outer_send, outer_recv.at[p * (chunks // WIDE) + c], (o, v_outer))

    def load(k):
        return pltpu.make_async_copy(b_ref.at[:, cols(k, WIDE)], own.at[:, cols(k, WIDE)], own_sem.at[k])

    barrier = pltpu.get_barrier_semaphore()
    for device in ((partner, v), (relay_to, v), (relay_from, v), (o, v_inner), (o, v_outer)):
        pl.semaphore_signal(barrier, inc=1, device_id=device, device_id_type=MESH)
    every(chunks // WIDE, lambda k: load(k).start())
    load(0).wait()
    pl.semaphore_wait(barrier, 5)
    for n in range(AHEAD):
        near_copy(0, n // pieces[0], n % pieces[0], own).start()
    for p in range(len(plan)):
        every(chunks // WIDE, lambda c: outer_copy(p, c).start())
        inner_copy(p).start()

    lane = lax.broadcasted_iota(jnp.int32, (8, rows), 1)

    def gap_row(base, count, blocks):
        part = min(count, vir_block)
        within = lax.rem(lane, part)
        virs = jnp.zeros((8, rows), jnp.float32)
        occs = virs
        for stream, (occ, vir) in enumerate(blocks):
            row = virs
            for a in range(part):
                row = jnp.where(within == a, vir_ref[vir * vir_block + base % vir_block + a], row)
            virs = jnp.where(lane >= stream * count, row, virs)
            for i in range(count // part):
                occs = jnp.where(
                    lane >= stream * count + i * part, occ_ref[occ * occ_block + base // vir_block + i], occs)
        return occs - virs

    def whole(row):
        return jnp.broadcast_to(row[:1], (rows, rows))

    own_row = gap_row(0, rows, [(o, v)])
    mine_gap[...] = whole(own_row).T

    def gather(block, k):
        count = block.shape[0]
        mine = (own_high[:, cols(k)], own_low[:, cols(k)])
        sums[:, :count] += product(mine, split(block), (1, 1))

    def amplitude(row, count):
        value = sums[:, :count] / (mine_gap[:, :count] + whole(row)[:, :count])
        high, low = split(value)
        amp_high[:, :count] = high
        if 2 * count <= DEPTH:
            amp_high[:, count:2 * count] = low
        else:
            amp_low[:, :count] = low
        sums[...] = jnp.zeros_like(sums)

    sums[...] = jnp.zeros_like(sums)

    def own_chunk(k):
        high, low = split(own[:, cols(k)])
        own_high[:, cols(k)] = high
        own_low[:, cols(k)] = low
        gather(own[:, cols(k)], k)

    def block(p, k):
        return land[pl.ds(STREAMS * plan[p][0], STREAMS * plan[p][1]), cols(k)]

    def read_first(p, k):
        if p == 0:
            total[:, cols(k)] = spread(amp_high, amp_low, own[:, cols(k)])
        else:
            total[:, cols(k)] += spread(amp_high, amp_low, block(p - 1, k))

    def read_second(p, k):
        def take_far(c):
            far_here(p, c).wait_recv()
            if far_first[p] < reused:
                pl.semaphore_signal(far_free, inc=1, device_id=(relay_from, v), device_id_type=MESH)

        if pairs[p] == 1:
            take_far(k)

        @pl.when(lax.rem(k, WIDE) == 0)
        def _():
            if pairs[p] == WIDE:
                take_far(k // WIDE)
            outer_copy(p, k // WIDE).wait_recv()
        gather(block(p, k), k)

    def finished(p):
        amplitude(gaps[p], STREAMS * plan[p][1])

    def relay(p, k, i):
        near_copy(p, k, i).wait_recv()
        if i == 0 and far_first[p] >= chunks:
            @pl.when(lax.rem(k, pairs[p]) == 0)
            def _():
                pl.semaphore_wait(far_free, 1)
        far_copy(p, k, i).start()
        later = chunks - AHEAD // pieces[p]

        @pl.when(k < later)
        def _():
            near_copy(p, k + AHEAD // pieces[p], i, own).start()

        if p + 1 < len(plan):
            ratio = pieces[p] // pieces[p + 1]

            @pl.when(k >= later)
            def _():
                near_copy(p + 1, (k - later) * ratio + i // pieces[p + 1], i % pieces[p + 1], own).start()

    def arrive(p, k, work):
        for i in range(pieces[p]):
            relay(p, k, i)
            if i < len(work):
                work[i]()

    def fill(p):
        gaps[p] = gap_row(plan[p][0], plan[p][1], sources)

    every(chunks // WIDE, lambda k: load(k).wait(), 1)

    slots = [functools.partial(every, k + 1, own_chunk, k) for k in range(chunks)]
    slots += [lambda: amplitude(own_row, rows)] + [functools.partial(fill, p) for p in range(len(plan))]
    for k in range(LAG):
        arrive(0, k, slots[k * pieces[0]:(k + 1) * pieces[0]])
    assert len(slots) <= LAG * pieces[0]

    done, runs = 0, []
    for p in range(len(plan)):
        for k in range(LAG if p == 0 else 0, chunks):
            due = p * chunks + k - LAG
            task = None
            if due >= done:
                task = done // chunks, done % chunks - k
                done += 1
            if runs and runs[-1][0] == p and runs[-1][3] == task:
                runs[-1][2] = k + 1
            else:
                runs.append([p, k, k + 1, task])

    for p, first, end, task in runs:
        if task is None:
            every(end, lambda k, p=p: arrive(p, k, []), first)
            continue
        q, shift = task
        if first + shift == 0:
            inner_copy(q).wait_recv()
        every(end, lambda k, p=p, q=q, shift=shift: arrive(
            p, k, [lambda: read_first(q, k + shift), lambda: read_second(q, k + shift)]), first)
        if end + shift == chunks:
            finished(q)

    while done < len(plan) * chunks:
        q, first = done // chunks, done % chunks
        if first == 0:
            inner_copy(q).wait_recv()

        def rest(k, q=q):
            read_first(q, k)
            read_second(q, k)
        every(chunks, rest, first)
        finished(q)
        done = (q + 1) * chunks

    sent = land.at[pl.ds(0, rows), :]
    remote(b_ref, sent, near_send, near_recv.at[0], (partner, v)).wait_send()
    remote(b_ref, sent, inner_send, inner_recv.at[0], (o, v_inner)).wait_send()
    remote(b_ref, sent, outer_send, outer_recv.at[0], (o, v_outer)).wait_send()
    remote(sent, sent, far_send, far_recv.at[0], (relay_to, v)).wait_send()


def finish(total, land, amp_high, amp_low, out_ref, done, out_sem):
    rows, width = total.shape
    base, count = phases(rows)[-1]
    stores = []
    for k in range(width // CHUNK):
        where = pl.ds(k * CHUNK, CHUNK)
        block = land[pl.ds(STREAMS * base, STREAMS * count), where]
        done[:, where] = total[:, where] + spread(amp_high, amp_low, block)
        stores.append(pltpu.make_async_copy(done.at[:, where], out_ref.at[:, where], out_sem.at[k]))
        stores[-1].start()
    for store in stores:
        store.wait()


def local(b_factors, occ_energy, vir_energy):
    occ_block, vir_block, width = b_factors.shape
    occ_count = lax.axis_size("occ")
    vir_count = lax.axis_size("vir")
    rows = occ_block * vir_block
    plan = phases(rows)
    chunks = width // CHUNK
    block = pltpu.VMEM((rows, width), jnp.float32)
    half = pltpu.VMEM((rows, width), jnp.bfloat16)
    square = pltpu.VMEM((rows, rows), jnp.float32)
    amp = pltpu.VMEM((rows, rows), jnp.bfloat16)
    vmem = pl.BlockSpec(memory_space=pltpu.VMEM)
    smem = pl.BlockSpec(memory_space=pltpu.SMEM)
    hbm = pl.BlockSpec(memory_space=pl.ANY)
    sems = [pltpu.SemaphoreType.REGULAR, pltpu.SemaphoreType.DMA((chunks // WIDE,))] + [pltpu.SemaphoreType.DMA] * 4 + [
        pltpu.SemaphoreType.DMA((count,))
        for count in (2 * AHEAD, chunks, len(plan), len(plan) * chunks // WIDE)]
    parts = pl.pallas_call(
        functools.partial(kernel, occ_count, vir_count, occ_block, vir_block),
        out_shape=[block, pltpu.VMEM((STREAMS * rows, width), jnp.float32), amp, amp],
        in_specs=[smem, smem, hbm],
        out_specs=[vmem] * 4,
        scratch_shapes=[
            block, half, half, square, square, pltpu.VMEM((len(plan), 8, rows), jnp.float32)] + sems,
        compiler_params=pltpu.CompilerParams(
            collective_id=0, has_side_effects=True, vmem_limit_bytes=42 * 2**20),
    )(occ_energy, vir_energy, b_factors.reshape(rows, width))
    out = pl.pallas_call(
        finish,
        out_shape=jax.ShapeDtypeStruct((rows, width), jnp.float32),
        in_specs=[vmem] * 4,
        out_specs=hbm,
        scratch_shapes=[block, pltpu.SemaphoreType.DMA((chunks,))],
        compiler_params=pltpu.CompilerParams(vmem_limit_bytes=10 * 2**20),
    )(*parts)
    return out.reshape(occ_block, vir_block, width)


def solution(mesh):
    in_specs = (P("occ", "vir", None), P(), P())
    out_specs = P("occ", "vir", None)
    return jax.shard_map(local, mesh=mesh, in_specs=in_specs, out_specs=out_specs, check_vma=False)
```

```python
import functools

import jax
import jax.numpy as jnp
from jax import lax
from jax.experimental import pallas as pl
from jax.experimental.pallas import tpu as pltpu
from jax.sharding import PartitionSpec as P

MESH = pl.DeviceIdType.MESH
CHUNK = 512
STREAMS = 4
SHARES = (4, 4, 4, 8, 8)
LAG = 5
RELAY_ROWS = 16
AHEAD = 8
WIDE = 2
DEPTH = 256


def phases(rows):
    out, base = [], 0
    for share in SHARES:
        out.append((base, rows // share))
        base += rows // share
    assert base == rows
    return out


def split(value):
    high = value.astype(jnp.bfloat16)
    low = (value - high.astype(jnp.float32)).astype(jnp.bfloat16)
    return high, low


def dot(a, b, contract):
    dims = ((contract[:1], contract[1:]), ((), ()))
    return lax.dot_general(a, b, dimension_numbers=dims, preferred_element_type=jnp.float32)


def product(a, b, contract):
    (a_high, a_low), (b_high, b_low) = a, b
    return dot(a_high, b_high, contract) + (dot(a_high, b_low, contract) + dot(a_low, b_high, contract))


def spread(amp_high, amp_low, block):
    count = block.shape[0]
    high, low = split(block)
    if 2 * count <= DEPTH:
        return dot(amp_high[:, :2 * count], jnp.concatenate([high, high], axis=0), (1, 0)) + dot(
            amp_high[:, :count], low, (1, 0))
    return product((amp_high[:, :count], amp_low[:, :count]), (high, low), (1, 0))


def cols(k, wide=1):
    size = wide * CHUNK
    return pl.ds(pl.multiple_of(k * size, size), size)


def every(count, body, first=0):
    def run(k, carry):
        body(k)
        return carry
    lax.fori_loop(first, count, run, 0)


def kernel(
    occ_count, vir_count, occ_block, vir_block,
    occ_ref, vir_ref, b_ref, total, land, amp_high, amp_low,
    own, own_high, own_low, sums, mine_gap, gaps,
    far_free, own_sem, near_send, far_send, inner_send, outer_send, near_recv, far_recv, inner_recv, outer_recv,
):
    rows, width = b_ref.shape
    plan = phases(rows)
    chunks = width // CHUNK
    o = lax.axis_index("occ")
    v = lax.axis_index("vir")
    step = 1 - 2 * lax.rem(o, 2)
    partner = o + step
    relay_to = lax.rem(o + 2 * step + occ_count, occ_count)
    relay_from = lax.rem(o - 2 * step + occ_count, occ_count)
    across = lax.rem(o - step + occ_count, occ_count)
    turn = 1 - 2 * lax.rem(v, 2)
    v_inner = v + turn
    v_outer = lax.rem(v - turn + vir_count, vir_count)
    sources = ((partner, v), (o, v_inner), (o, v_outer), (across, v))
    pieces = [count // RELAY_ROWS for _, count in plan]
    pairs = [WIDE if count > min(c for _, c in plan) else 1 for _, count in plan]
    far_first = [sum(chunks // pair for pair in pairs[:p]) for p in range(len(plan) + 1)]
    reused = far_first[-1] - chunks
    assert chunks in far_first and reused in far_first

    def mine(p, i, count, where, ref=b_ref):
        return ref.at[pl.ds(plan[p][0] + i * count, count), where]

    def landed(p, stream, i, count, where):
        return land.at[pl.ds(STREAMS * plan[p][0] + stream * plan[p][1] + i * count, count), where]

    def remote(source, target, send_sem, recv_sem, device):
        return pltpu.make_async_remote_copy(
            source, target, send_sem, recv_sem, device_id=device, device_id_type=MESH)

    def near_copy(p, k, i, ref=b_ref):
        return remote(
            mine(p, i, RELAY_ROWS, cols(k), ref), landed(p, 0, i, RELAY_ROWS, cols(k)),
            near_send, near_recv.at[lax.rem(k * pieces[p] + i, 2 * AHEAD)], (partner, v))

    def far_copy(p, k, i):
        return remote(
            landed(p, 0, i, RELAY_ROWS, cols(k)), landed(p, 3, i, RELAY_ROWS, cols(k)),
            far_send, far_recv.at[lax.rem(far_first[p] + k // pairs[p], chunks)], (relay_to, v))

    def far_here(p, c):
        where = cols(c, pairs[p])
        return remote(
            landed(p, 0, 0, plan[p][1], where), landed(p, 3, 0, plan[p][1], where),
            far_send, far_recv.at[lax.rem(far_first[p] + c, chunks)], (relay_to, v))

    def inner_copy(p):
        count = plan[p][1]
        return remote(
            mine(p, 0, count, slice(None)), landed(p, 1, 0, count, slice(None)),
            inner_send, inner_recv.at[p], (o, v_inner))

    def outer_copy(p, c):
        count = plan[p][1]
        return remote(
            mine(p, 0, count, cols(c, WIDE)), landed(p, 2, 0, count, cols(c, WIDE)),
            outer_send, outer_recv.at[p * (chunks // WIDE) + c], (o, v_outer))

    def load(k):
        return pltpu.make_async_copy(b_ref.at[:, cols(k, WIDE)], own.at[:, cols(k, WIDE)], own_sem.at[jnp.minimum(k, 1)])

    barrier = pltpu.get_barrier_semaphore()
    for device in ((partner, v), (relay_to, v), (relay_from, v), (o, v_inner), (o, v_outer)):
        pl.semaphore_signal(barrier, inc=1, device_id=device, device_id_type=MESH)
    every(chunks // WIDE, lambda k: load(k).start())
    load(0).wait()
    pl.semaphore_wait(barrier, 5)
    for n in range(AHEAD):
        near_copy(0, n // pieces[0], n % pieces[0], own).start()
    for p in range(len(plan)):
        every(chunks // WIDE, lambda c: outer_copy(p, c).start())
        inner_copy(p).start()

    lane = lax.broadcasted_iota(jnp.int32, (8, rows), 1)

    def gap_row(base, count, blocks):
        part = min(count, vir_block)
        within = lax.rem(lane, part)
        virs = jnp.zeros((8, rows), jnp.float32)
        occs = virs
        for stream, (occ, vir) in enumerate(blocks):
            row = virs
            for a in range(part):
                row = jnp.where(within == a, vir_ref[vir * vir_block + base % vir_block + a], row)
            virs = jnp.where(lane >= stream * count, row, virs)
            for i in range(count // part):
                occs = jnp.where(
                    lane >= stream * count + i * part, occ_ref[occ * occ_block + base // vir_block + i], occs)
        return occs - virs

    def whole(row):
        return jnp.broadcast_to(row[:1], (rows, rows))

    own_row = gap_row(0, rows, [(o, v)])
    mine_gap[...] = whole(own_row).T

    def gather(block, k):
        count = block.shape[0]
        mine = (own_high[:, cols(k)], own_low[:, cols(k)])
        sums[:, :count] += product(mine, split(block), (1, 1))

    def amplitude(row, count, last=False):
        value = sums[:, :count] / (mine_gap[:, :count] + whole(row)[:, :count])
        high, low = split(value)
        amp_high[:, :count] = high
        if 2 * count <= DEPTH:
            amp_high[:, count:2 * count] = low
        else:
            amp_low[:, :count] = low
        if not last:
            sums[...] = jnp.zeros_like(sums)

    sums[...] = jnp.zeros_like(sums)

    def own_chunk(k):
        high, low = split(own[:, cols(k)])
        own_high[:, cols(k)] = high
        own_low[:, cols(k)] = low
        gather(own[:, cols(k)], k)

    def block(p, k):
        return land[pl.ds(STREAMS * plan[p][0], STREAMS * plan[p][1]), cols(k)]

    def read_first(p, k):
        if p == 0:
            total[:, cols(k)] = spread(amp_high, amp_low, own[:, cols(k)])
        else:
            total[:, cols(k)] += spread(amp_high, amp_low, block(p - 1, k))

    def read_second(p, k):
        def take_far(c):
            far_here(p, c).wait_recv()
            if far_first[p] < reused:
                pl.semaphore_signal(far_free, inc=1, device_id=(relay_from, v), device_id_type=MESH)

        if pairs[p] == 1:
            take_far(k)

        @pl.when(lax.rem(k, WIDE) == 0)
        def _():
            if pairs[p] == WIDE:
                take_far(k // WIDE)
            outer_copy(p, k // WIDE).wait_recv()
        gather(block(p, k), k)

    def finished(p):
        amplitude(gaps[p], STREAMS * plan[p][1], p == len(plan) - 1)

    def relay(p, k, i):
        near_copy(p, k, i).wait_recv()
        if i == 0 and far_first[p] >= chunks:
            @pl.when(lax.rem(k, pairs[p]) == 0)
            def _():
                pl.semaphore_wait(far_free, 1)
        far_copy(p, k, i).start()
        later = chunks - AHEAD // pieces[p]

        @pl.when(k < later)
        def _():
            near_copy(p, k + AHEAD // pieces[p], i, own).start()

        if p + 1 < len(plan):
            ratio = pieces[p] // pieces[p + 1]

            @pl.when(k >= later)
            def _():
                near_copy(p + 1, (k - later) * ratio + i // pieces[p + 1], i % pieces[p + 1], own).start()

    def arrive(p, k, work):
        for i in range(pieces[p]):
            relay(p, k, i)
            if i < len(work):
                work[i]()

    def fill(p):
        gaps[p] = gap_row(plan[p][0], plan[p][1], sources)

    others = pl.ds(WIDE * CHUNK, width - WIDE * CHUNK)
    pltpu.make_async_copy(b_ref.at[:, others], own.at[:, others], own_sem.at[1]).wait()

    slots = [functools.partial(every, k + 1, own_chunk, k) for k in range(chunks)]
    slots += [lambda: amplitude(own_row, rows)] + [functools.partial(fill, p) for p in range(len(plan))]
    for k in range(LAG):
        arrive(0, k, slots[k * pieces[0]:(k + 1) * pieces[0]])
    assert len(slots) <= LAG * pieces[0]

    done, runs = 0, []
    for p in range(len(plan)):
        for k in range(LAG if p == 0 else 0, chunks):
            due = p * chunks + k - LAG
            task = None
            if due >= done:
                task = done // chunks, done % chunks - k
                done += 1
            if runs and runs[-1][0] == p and runs[-1][3] == task:
                runs[-1][2] = k + 1
            else:
                runs.append([p, k, k + 1, task])

    for p, first, end, task in runs:
        if task is None:
            every(end, lambda k, p=p: arrive(p, k, []), first)
            continue
        q, shift = task
        if first + shift == 0:
            inner_copy(q).wait_recv()
        every(end, lambda k, p=p, q=q, shift=shift: arrive(
            p, k, [lambda: read_first(q, k + shift), lambda: read_second(q, k + shift)]), first)
        if end + shift == chunks:
            finished(q)

    while done < len(plan) * chunks:
        q, first = done // chunks, done % chunks
        if first == 0:
            inner_copy(q).wait_recv()

        def rest(k, q=q):
            read_first(q, k)
            read_second(q, k)
        every(chunks, rest, first)
        finished(q)
        done = (q + 1) * chunks

    sent = land.at[pl.ds(0, rows), :]
    remote(b_ref, sent, near_send, near_recv.at[0], (partner, v)).wait_send()
    remote(b_ref, sent, inner_send, inner_recv.at[0], (o, v_inner)).wait_send()
    remote(b_ref, sent, outer_send, outer_recv.at[0], (o, v_outer)).wait_send()
    remote(sent, sent, far_send, far_recv.at[0], (relay_to, v)).wait_send()


def finish(total, land, amp_high, amp_low, out_ref, done, out_sem):
    rows, width = total.shape
    base, count = phases(rows)[-1]
    stores = []
    for k in range(width // CHUNK):
        where = pl.ds(k * CHUNK, CHUNK)
        block = land[pl.ds(STREAMS * base, STREAMS * count), where]
        done[:, where] = total[:, where] + spread(amp_high, amp_low, block)
        stores.append(pltpu.make_async_copy(done.at[:, where], out_ref.at[:, where], out_sem.at[k]))
        stores[-1].start()
    for store in stores:
        store.wait()


def local(b_factors, occ_energy, vir_energy):
    occ_block, vir_block, width = b_factors.shape
    occ_count = lax.axis_size("occ")
    vir_count = lax.axis_size("vir")
    rows = occ_block * vir_block
    plan = phases(rows)
    chunks = width // CHUNK
    block = pltpu.VMEM((rows, width), jnp.float32)
    half = pltpu.VMEM((rows, width), jnp.bfloat16)
    square = pltpu.VMEM((rows, rows), jnp.float32)
    amp = pltpu.VMEM((rows, rows), jnp.bfloat16)
    vmem = pl.BlockSpec(memory_space=pltpu.VMEM)
    smem = pl.BlockSpec(memory_space=pltpu.SMEM)
    hbm = pl.BlockSpec(memory_space=pl.ANY)
    sems = [pltpu.SemaphoreType.REGULAR, pltpu.SemaphoreType.DMA((2,))] + [pltpu.SemaphoreType.DMA] * 4 + [
        pltpu.SemaphoreType.DMA((count,))
        for count in (2 * AHEAD, chunks, len(plan), len(plan) * chunks // WIDE)]
    parts = pl.pallas_call(
        functools.partial(kernel, occ_count, vir_count, occ_block, vir_block),
        out_shape=[block, pltpu.VMEM((STREAMS * rows, width), jnp.float32), amp, amp],
        in_specs=[smem, smem, hbm],
        out_specs=[vmem] * 4,
        scratch_shapes=[
            block, half, half, square, square, pltpu.VMEM((len(plan), 8, rows), jnp.float32)] + sems,
        compiler_params=pltpu.CompilerParams(
            collective_id=0, has_side_effects=True, vmem_limit_bytes=42 * 2**20),
    )(occ_energy, vir_energy, b_factors.reshape(rows, width))
    out = pl.pallas_call(
        finish,
        out_shape=jax.ShapeDtypeStruct((rows, width), jnp.float32),
        in_specs=[vmem] * 4,
        out_specs=hbm,
        scratch_shapes=[block, pltpu.SemaphoreType.DMA((chunks,))],
        compiler_params=pltpu.CompilerParams(vmem_limit_bytes=10 * 2**20),
    )(*parts)
    return out.reshape(occ_block, vir_block, width)


def solution(mesh):
    in_specs = (P("occ", "vir", None), P(), P())
    out_specs = P("occ", "vir", None)
    return jax.shard_map(local, mesh=mesh, in_specs=in_specs, out_specs=out_specs, check_vma=False)
```
